32 devices in a mesh: batch: 16 (over z, y, core), rep: 2 (over x).
Axes of the slice: x: 2, y: 2, z: 4, core: 2. Of those that a mesh axis runs over, the one named last changes fastest.
Arguments:
- queries: bfloat16 [2048, 512], P('batch', 'rep'), may hold values from -8 to 8
- passages: bfloat16 [2048, 512], P('batch', 'rep'), may hold values from -8 to 8
- positives: int32 [2048], replicated, may hold values from 0 to 2047, each once
Outputs:
- grad_queries: float32 [2048, 512], P('batch', 'rep')
- grad_passages: float32 [2048, 512], P('batch', 'rep')
The draws below stay inside these ranges and needn't reach their ends.
Inputs may be any that keep to these rules, and one draw needn't show every extreme that they name: `positives`: each passage is the positive of exactly one query.
All inputs are finite; a program needn't handle non-finite values.
Results may differ from the reference program's by a relative error of at most 0.0013.
Values may be sent and summed in bfloat16 or wider, within the bound.
A program may use at most 128 MiB of HBM per device.

```python
import math
import jax
import jax.numpy as jnp
from jax import lax

D = 512
TOTAL = 2048


def embedding_draw(key, member):
    member_key = jax.random.fold_in(key, member + 11)
    scale_key, entry_key = jax.random.split(member_key, 2)
    row_scale = jnp.exp(jax.random.uniform(scale_key, (TOTAL, 1), jnp.float32, math.log(0.3), math.log(3.0)))
    entries = jax.random.normal(entry_key, (TOTAL, D), jnp.float32)
    values = jnp.clip(row_scale * entries, -8.0, 8.0)
    return values.astype(jnp.bfloat16)


def draw_queries(key, part):
    return embedding_draw(key, 0)


def draw_passages(key, part):
    return embedding_draw(key, 1)


def setup_inputs(seed: int = 0) -> dict:
    key_list = jax.random.split(jax.random.key(seed), 4)
    return {
        "queries": draw_queries(jax.random.fold_in(key_list[3], 71), 0),
        "passages": draw_passages(jax.random.fold_in(key_list[3], 71), 0),
        "positives": jax.random.permutation(key_list[2], TOTAL).astype(jnp.int32),
    }


def block_scores(query_block, passages, logit_scale):
    return jnp.dot(query_block, passages.T, preferred_element_type=jnp.float32) * logit_scale

def reference(queries, passages, positives):
    logit_scale = 1.0 / math.sqrt(D)
    block_rows = math.gcd(TOTAL, 512)
    block_count = TOTAL // block_rows
    query_blocks = queries.reshape(block_count, block_rows, D)
    positive_blocks = positives.reshape(block_count, block_rows)

    def first_sweep(running, query_block):
        column_high, column_total = running
        scores = block_scores(query_block, passages, logit_scale)
        row_high = lax.optimization_barrier(jnp.max(scores, axis=1))
        row_norm = row_high + jnp.log(lax.optimization_barrier(jnp.sum(jnp.exp(scores - row_high[:, None]), axis=1)))
        new_high = jnp.maximum(column_high, lax.optimization_barrier(jnp.max(scores, axis=0)))
        column_total = column_total * jnp.exp(column_high - new_high) + lax.optimization_barrier(jnp.sum(jnp.exp(scores - new_high[None, :]), axis=0))
        return ((new_high, column_total), row_norm)
    starting = (jnp.full((TOTAL,), -1e+30, jnp.float32), jnp.zeros((TOTAL,), jnp.float32))
    (column_high, column_total), row_norms = lax.scan(first_sweep, starting, query_blocks)
    column_norms = column_high + jnp.log(column_total)
    passage_ids = jnp.arange(TOTAL, dtype=jnp.int32)

    def second_sweep(grad_passages, inputs):
        query_block, row_block, positive_block = inputs
        scores = block_scores(query_block, passages, logit_scale)
        matches = (positive_block[:, None] == passage_ids[None, :]).astype(jnp.float32)
        weights = jnp.exp(scores - row_block[:, None]) + jnp.exp(scores - column_norms[None, :]) - 2.0 * matches
        weights = weights.astype(jnp.bfloat16)
        grad_block = jnp.dot(weights, passages, preferred_element_type=jnp.float32) * logit_scale
        grad_passages = grad_passages + jnp.dot(weights.T, query_block, preferred_element_type=jnp.float32) * logit_scale
        return (grad_passages, grad_block)
    grad_passages, grad_blocks = lax.scan(second_sweep, jnp.zeros((TOTAL, D), jnp.float32), (query_blocks, row_norms, positive_blocks))
    return (grad_blocks.reshape(TOTAL, D), grad_passages)
```

```python
import functools
import math

import jax
import jax.numpy as jnp
from jax import lax
from jax.experimental import pallas as pl
from jax.experimental.pallas import tpu as pltpu
from jax.sharding import PartitionSpec as P

MESH = pl.DeviceIdType.MESH
F32 = jnp.float32
BF16 = jnp.bfloat16


def dot(a, b, da, db):
    return lax.dot_general(a, b, (((da,), (db,)), ((), ())), preferred_element_type=F32)


def as_column(row, lanes):
    return jnp.broadcast_to(row, (lanes, row.shape[1])).T


def kernel(
    Z,
    scale,
    q_ref,
    p_ref,
    pos_ref,
    gq_ref,
    gp_ref,
    Q,
    Qs,
    PB,
    S,
    W,
    Ws,
    rst,
    rrc,
    cst,
    crc,
    gqp,
    gqr,
    gpp,
    gpr,
    q_s,
    q_r,
    p_s,
    p_r,
    f_s,
    f_r,
    h_s,
    h_r,
    r_s,
    r_r,
    c_s,
    c_r,
    w_s,
    w_r,
    gq_s,
    gq_r,
    gp_s,
    gp_r,
):
    n, w = q_ref.shape
    b = lax.axis_index("batch")
    x = lax.axis_index("rep")
    z, y, c = b // 4, (b // 2) % 2, b % 2
    rows, cols = 2 * n, Z * n
    blocks = min(Z, 4)
    wide = blocks * n
    chunks = Z // blocks

    def dev(zz, yy, cc, xx):
        return (zz * 4 + yy * 2 + cc, xx)

    def plane(j):
        xx = 1 - x if j & 1 else x
        yy = 1 - y if j & 2 else y
        return xx, yy

    def remote(src, dst, s, r, device):
        return pltpu.make_async_remote_copy(
            src_ref=src, dst_ref=dst, send_sem=s, recv_sem=r, device_id=device, device_id_type=MESH
        )

    def up(dz):
        return (z + dz) % Z

    def down(dz):
        return (z + Z - dz) % Z

    own = c == x
    sibling = dev(z, y, 1 - c, x)

    barrier = pltpu.get_barrier_semaphore()

    def greet(device):
        pl.semaphore_signal(barrier, inc=1, device_id=device, device_id_type=MESH)

    for j in (1, 2, 3):
        xx, yy = plane(j)
        greet(dev(z, yy, c, xx))
    for dz in range(Z):
        if dz:
            greet(dev(up(dz), y, c, x))
            greet(dev(up(dz), y, x, c))
        else:

            @pl.when(jnp.logical_not(own))
            def _():
                greet(dev(z, y, x, c))

        greet(dev(up(dz), y, 1 - c, x))
    Q[x, pl.ds(pl.multiple_of(y * n, n), n), :] = q_ref[...]

    @pl.when(own)
    def _():
        PB[c, pl.ds(pl.multiple_of(z * n, n), n), :] = p_ref[...]

    pl.semaphore_wait(barrier, 3 + 3 * Z - 1 - own.astype(jnp.int32))

    def p_copy(dz, dst_z):
        return remote(
            p_ref,
            PB.at[x, pl.ds(pl.multiple_of(dst_z * n, n), n)],
            p_s.at[dz],
            p_r.at[dz],
            dev(up(dz), y, x, c),
        )

    def q_copy(j):
        xx, yy = plane(j)
        return remote(
            q_ref,
            Q.at[x, pl.ds(pl.multiple_of(y * n, n), n)],
            q_s.at[j - 1],
            q_r.at[j - 1],
            dev(z, yy, c, xx),
        )

    p_copies = [p_copy(dz, z) for dz in range(Z)]
    q_copies = [q_copy(j) for j in (1, 2, 3)]
    forward0 = remote(
        p_ref,
        PB.at[c, pl.ds(pl.multiple_of(z * n, n), n)],
        f_s.at[0],
        f_r.at[0],
        sibling,
    )

    @pl.when(jnp.logical_not(own))
    def _():
        p_copies[0].start()

    @pl.when(own)
    def _():
        forward0.start()

    order = list(range(1, Z))
    for dz in order:
        p_copies[dz].start()
    for copy in q_copies:
        copy.start()

    def forward(dz):
        zs = down(dz)
        part = PB.at[c, pl.ds(pl.multiple_of(zs * n, n), n)]
        return remote(part, part, f_s.at[dz], f_r.at[dz], sibling)

    forwards = [forward(dz) for dz in range(Z)]

    for copy in q_copies:
        copy.wait_recv()
    half = remote(Q.at[1 - c], Qs, h_s, h_r, sibling)
    half.start()

    @pl.when(jnp.logical_not(own))
    def _():
        p_copies[0].wait_recv()
        forwards[0].start()

    for dz in order:
        p_copies[dz].wait_recv()
        forwards[dz].start()
    for dz in range(Z):
        forwards[dz].wait_recv()

    def span(k, size):
        return pl.ds(k * size if isinstance(k, int) else pl.multiple_of(k * size, size), size)

    def score(k, running):
        high, total = running
        at = span(k, wide)
        s = (dot(Q[0], PB[0, at, :], 1, 1) + dot(Q[1], PB[1, at, :], 1, 1)) * scale
        S[:, at] = s
        top = jnp.max(s, axis=0, keepdims=True)
        cst[:, at] = top
        cst[:, span(k + chunks, wide)] = jnp.sum(jnp.exp(s - top), axis=0, keepdims=True)
        new = jnp.maximum(high, jnp.max(s, axis=1, keepdims=True))
        total = total * jnp.exp(high - new) + jnp.sum(jnp.exp(s - new), axis=1, keepdims=True)
        return new, total

    running = (jnp.full((rows, 1), -1e30, F32), jnp.zeros((rows, 1), F32))
    if chunks == 1:
        running = score(0, running)
    else:
        running = lax.fori_loop(0, chunks, score, running)

    col_copies = []
    for dz in range(Z):
        for dc in (0, 1):
            if dz or dc:
                k = dz * 2 + dc
                col_copies.append(
                    remote(
                        cst,
                        crc.at[k],
                        c_s.at[k],
                        c_r.at[k],
                        dev(up(dz), y, 1 - c if dc else c, x),
                    )
                )
                col_copies[-1].start()

    def as_row(column):
        return jnp.broadcast_to(column, (rows, 128)).T[0:1, :]

    rst[:, 0:rows] = as_row(running[0])
    rst[:, rows : 2 * rows] = as_row(running[1])
    row_copies = []
    for j in (1, 2, 3):
        xx, yy = plane(j)
        row_copies.append(
            remote(rst, rrc.at[j], r_s.at[j - 1], r_r.at[j - 1], dev(z, yy, c, xx))
        )
        row_copies[-1].start()

    places = jnp.concatenate(
        [
            as_column(pos_ref[pl.ds(z * 4 + yy * 2 + c, 1), :].astype(F32), 128)
            for yy in (0, 1)
        ],
        axis=0,
    )

    for copy in row_copies:
        copy.wait_recv()
    high = rst[:, 0:rows]
    for j in (1, 2, 3):
        high = jnp.maximum(high, rrc[j, :, 0:rows])
    total = rst[:, rows : 2 * rows] * jnp.exp(rst[:, 0:rows] - high)
    for j in (1, 2, 3):
        total += rrc[j, :, rows : 2 * rows] * jnp.exp(rrc[j, :, 0:rows] - high)
    row_norm = as_column(high + jnp.log(total), 128)

    for copy in col_copies:
        copy.wait_recv()
    high = cst[:, 0:cols]
    for k in range(1, 2 * Z):
        high = jnp.maximum(high, crc[k, :, 0:cols])
    total = cst[:, cols : 2 * cols] * jnp.exp(cst[:, 0:cols] - high)
    for k in range(1, 2 * Z):
        total += crc[k, :, cols : 2 * cols] * jnp.exp(crc[k, :, 0:cols] - high)
    crc[0, :, 0:cols] = high + jnp.log(total)

    lane = lax.broadcasted_iota(jnp.int32, (rows, n), 1).astype(F32)

    def weigh(k, carry):
        at = span(k, n)
        s = S[:, at]
        col_norm = crc[0, :, at]
        base = (k * 4 + y * 2 + x) * n
        hit = jnp.where(places - lane == lax.convert_element_type(base, F32), 2.0, 0.0)
        W[:, at] = (jnp.exp(s - row_norm) + jnp.exp(s - col_norm) - hit).astype(BF16)
        return carry

    if chunks == 1:
        for k in range(Z):
            weigh(k, 0)
    else:
        lax.fori_loop(0, Z, weigh, 0)
    share = remote(W, Ws, w_s, w_r, sibling)
    share.start()

    if chunks == 1:
        for h in (0, 1):
            gqp[h] = dot(W[...], PB[h], 1, 0)
    else:
        gqp[...] = jnp.zeros_like(gqp)

        def gather_terms(k, carry):
            at = span(k, wide)
            for h in (0, 1):
                gqp[h] += dot(W[:, at], PB[h, at, :], 1, 0)
            return carry

        lax.fori_loop(0, chunks, gather_terms, 0)
    gq_copies = []
    for j in (1, 2, 3):
        xx, yy = plane(j)
        gq_copies.append(
            remote(
                gqp.at[xx, pl.ds(pl.multiple_of(yy * n, n), n)],
                gqr.at[j - 1],
                gq_s.at[j - 1],
                gq_r.at[j - 1],
                dev(z, yy, c, xx),
            )
        )
        gq_copies[-1].start()

    half.wait_recv()
    share.wait_recv()

    def passage_terms(k, carry):
        at = span(k, wide)
        gpp[at, :] = dot(W[:, at], Q[c], 0, 0) + dot(Ws[:, at], Qs[...], 0, 0)
        return carry

    if chunks == 1:
        passage_terms(0, 0)
    else:
        lax.fori_loop(0, chunks, passage_terms, 0)

    def gp_copy(dz):
        return remote(
            gpp.at[pl.ds(pl.multiple_of(up(dz) * n, n), n)],
            gpr.at[dz],
            gp_s.at[dz],
            gp_r.at[dz],
            dev(up(dz), y, x, c),
        )

    gp_copies = [gp_copy(dz) for dz in range(Z)]
    for dz in order:
        gp_copies[dz].start()

    @pl.when(jnp.logical_not(own))
    def _():
        gp_copies[0].start()

    for copy in gq_copies:
        copy.wait_recv()
    total = gqp[x, pl.ds(pl.multiple_of(y * n, n), n), :]
    for j in range(3):
        total += gqr[j]
    gq_ref[...] = total * scale

    @pl.when(own)
    def _():
        gpr[0] = gpp[pl.ds(pl.multiple_of(z * n, n), n), :]

    @pl.when(jnp.logical_not(own))
    def _():
        gp_copies[0].wait_recv()

    for dz in order:
        gp_copies[dz].wait_recv()
    total = gpr[0]
    for dz in range(1, Z):
        total += gpr[dz]
    gp_ref[...] = total * scale

    @pl.when(jnp.logical_not(own))
    def _():
        p_copies[0].wait_send()
        gp_copies[0].wait_send()

    for dz in order:
        p_copies[dz].wait_send()
        gp_copies[dz].wait_send()
    for copy in q_copies + forwards + [half, share] + col_copies + row_copies + gq_copies:
        copy.wait_send()


def local(queries, passages, positives):
    n, w = queries.shape
    batch_count = lax.axis_size("batch")
    Z = batch_count // 4
    scale = 1.0 / math.sqrt(w * lax.axis_size("rep"))
    rows, cols = 2 * n, Z * n
    vmem = pl.BlockSpec(memory_space=pltpu.VMEM)
    dma = pltpu.SemaphoreType.DMA
    return pl.pallas_call(
        functools.partial(kernel, Z, scale),
        out_shape=(
            jax.ShapeDtypeStruct((n, w), F32),
            jax.ShapeDtypeStruct((n, w), F32),
        ),
        in_specs=[vmem] * 3,
        out_specs=(vmem, vmem),
        scratch_shapes=[
            pltpu.VMEM((2, rows, w), BF16),
            pltpu.VMEM((rows, w), BF16),
            pltpu.VMEM((2, cols, w), BF16),
            pltpu.VMEM((rows, cols), F32),
            pltpu.VMEM((rows, cols), BF16),
            pltpu.VMEM((rows, cols), BF16),
            pltpu.VMEM((1, 2 * rows), F32),
            pltpu.VMEM((4, 1, 2 * rows), F32),
            pltpu.VMEM((1, 2 * cols), F32),
            pltpu.VMEM((2 * Z, 1, 2 * cols), F32),
            pltpu.VMEM((2, rows, w), F32),
            pltpu.VMEM((3, n, w), F32),
            pltpu.VMEM((cols, w), F32),
            pltpu.VMEM((Z, n, w), F32),
            dma((3,)),
            dma((3,)),
            dma((Z,)),
            dma((Z,)),
            dma((Z,)),
            dma((Z,)),
            dma,
            dma,
            dma((3,)),
            dma((3,)),
            dma((2 * Z,)),
            dma((2 * Z,)),
            dma,
            dma,
            dma((3,)),
            dma((3,)),
            dma((Z,)),
            dma((Z,)),
        ],
        compiler_params=pltpu.CompilerParams(collective_id=0, has_side_effects=True),
    )(queries, passages, positives.reshape(batch_count, n))


def solution(mesh):
    in_specs = (P("batch", "rep"), P("batch", "rep"), P())
    out_specs = (P("batch", "rep"), P("batch", "rep"))
    return jax.shard_map(local, mesh=mesh, in_specs=in_specs, out_specs=out_specs, check_vma=False)
```

```python
import functools
import math

import jax
import jax.numpy as jnp
from jax import lax
from jax.experimental import pallas as pl
from jax.experimental.pallas import tpu as pltpu
from jax.sharding import PartitionSpec as P

MESH = pl.DeviceIdType.MESH
F32 = jnp.float32
BF16 = jnp.bfloat16
I16 = jnp.int16


def dot(a, b, da, db):
    return lax.dot_general(a, b, (((da,), (db,)), ((), ())), preferred_element_type=F32)


def as_column(row, lanes):
    return jnp.broadcast_to(row, (lanes, row.shape[1])).T


def kernel(
    Z,
    scale,
    q_ref,
    p_ref,
    pos_ref,
    gq_ref,
    gp_ref,
    Q,
    Qs,
    PB,
    S,
    W,
    Ws,
    rst,
    rrc,
    cst,
    crc,
    PM,
    gqp,
    gqt,
    gqr,
    gqk,
    gqkr,
    gpp,
    gpt,
    gpr,
    gpk,
    gpkr,
    fin,
    q_s,
    q_r,
    p_s,
    p_r,
    f_s,
    f_r,
    h_s,
    h_r,
    r_s,
    r_r,
    c_s,
    c_r,
    w_s,
    w_r,
    gq_s,
    gq_r,
    gp_s,
    gp_r,
    gqk_s,
    gqk_r,
    gpk_s,
    gpk_r,
    in_s,
):
    n, w = q_ref.shape
    b = lax.axis_index("batch")
    x = lax.axis_index("rep")
    z, y, c = b // 4, (b // 2) % 2, b % 2
    rows, cols = 2 * n, Z * n
    blocks = min(Z, 4)
    wide = blocks * n
    chunks = Z // blocks

    def dev(zz, yy, cc, xx):
        return (zz * 4 + yy * 2 + cc, xx)

    def plane(j):
        xx = 1 - x if j & 1 else x
        yy = 1 - y if j & 2 else y
        return xx, yy

    def remote(src, dst, s, r, device):
        return pltpu.make_async_remote_copy(
            src_ref=src, dst_ref=dst, send_sem=s, recv_sem=r, device_id=device, device_id_type=MESH
        )

    def up(dz):
        return (z + dz) % Z

    def down(dz):
        return (z + Z - dz) % Z

    own = c == x
    sibling = dev(z, y, 1 - c, x)

    barrier = pltpu.get_barrier_semaphore()

    q_own = Q.at[x, pl.ds(pl.multiple_of(y * n, n), n)]
    p_in = pltpu.make_async_copy(p_ref, PM, in_s.at[0])
    q_in = pltpu.make_async_copy(q_ref, q_own, in_s.at[1])
    p_in.start()
    q_in.start()

    def greet(device):
        pl.semaphore_signal(barrier, inc=1, device_id=device, device_id_type=MESH)

    for j in (1, 2, 3):
        xx, yy = plane(j)
        greet(dev(z, yy, c, xx))
    for dz in range(Z):
        if dz:
            greet(dev(up(dz), y, c, x))
            greet(dev(up(dz), y, x, c))
        else:

            @pl.when(jnp.logical_not(own))
            def _():
                greet(dev(z, y, x, c))

        greet(dev(up(dz), y, 1 - c, x))
    p_in.wait()
    q_in.wait()

    @pl.when(own)
    def _():
        PB[c, pl.ds(pl.multiple_of(z * n, n), n), :] = PM[...]

    pl.semaphore_wait(barrier, 3 + 3 * Z - 1 - own.astype(jnp.int32))

    def p_copy(dz, dst_z):
        return remote(
            PM,
            PB.at[x, pl.ds(pl.multiple_of(dst_z * n, n), n)],
            p_s.at[dz],
            p_r.at[dz],
            dev(up(dz), y, x, c),
        )

    def q_copy(j):
        xx, yy = plane(j)
        return remote(
            q_own,
            q_own,
            q_s.at[j - 1],
            q_r.at[j - 1],
            dev(z, yy, c, xx),
        )

    p_copies = [p_copy(dz, z) for dz in range(Z)]
    q_copies = [q_copy(j) for j in (1, 2, 3)]
    forward0 = remote(
        PM,
        PB.at[c, pl.ds(pl.multiple_of(z * n, n), n)],
        f_s.at[0],
        f_r.at[0],
        sibling,
    )

    @pl.when(jnp.logical_not(own))
    def _():
        p_copies[0].start()

    @pl.when(own)
    def _():
        forward0.start()

    order = list(range(1, Z))
    for dz in order:
        p_copies[dz].start()
    for copy in q_copies:
        copy.start()

    def forward(dz):
        zs = down(dz)
        part = PB.at[c, pl.ds(pl.multiple_of(zs * n, n), n)]
        return remote(part, part, f_s.at[dz], f_r.at[dz], sibling)

    forwards = [forward(dz) for dz in range(Z)]

    for copy in q_copies:
        copy.wait_recv()
    half = remote(Q.at[1 - c], Qs, h_s, h_r, sibling)
    half.start()

    @pl.when(jnp.logical_not(own))
    def _():
        p_copies[0].wait_recv()
        forwards[0].start()

    for dz in order:
        p_copies[dz].wait_recv()
        forwards[dz].start()
    for dz in range(Z):
        forwards[dz].wait_recv()

    def span(k, size):
        return pl.ds(k * size if isinstance(k, int) else pl.multiple_of(k * size, size), size)

    def score(k, running):
        high, total = running
        at = span(k, wide)
        s = (dot(Q[0], PB[0, at, :], 1, 1) + dot(Q[1], PB[1, at, :], 1, 1)) * scale
        S[:, at] = s
        top = jnp.max(s, axis=0, keepdims=True)
        cst[:, at] = top
        cst[:, span(k + chunks, wide)] = jnp.sum(jnp.exp(s - top), axis=0, keepdims=True)
        new = jnp.maximum(high, jnp.max(s, axis=1, keepdims=True))
        total = total * jnp.exp(high - new) + jnp.sum(jnp.exp(s - new), axis=1, keepdims=True)
        return new, total

    running = (jnp.full((rows, 1), -1e30, F32), jnp.zeros((rows, 1), F32))
    if chunks == 1:
        running = score(0, running)
    else:
        running = lax.fori_loop(0, chunks, score, running)

    col_copies = []
    for dz in range(Z):
        for dc in (0, 1):
            if dz or dc:
                k = dz * 2 + dc
                col_copies.append(
                    remote(
                        cst,
                        crc.at[k],
                        c_s.at[k],
                        c_r.at[k],
                        dev(up(dz), y, 1 - c if dc else c, x),
                    )
                )
                col_copies[-1].start()

    def as_row(column):
        return jnp.broadcast_to(column, (rows, 128)).T[0:1, :]

    rst[:, 0:rows] = as_row(running[0])
    rst[:, rows : 2 * rows] = as_row(running[1])
    row_copies = []
    for j in (1, 2, 3):
        xx, yy = plane(j)
        row_copies.append(
            remote(rst, rrc.at[j], r_s.at[j - 1], r_r.at[j - 1], dev(z, yy, c, xx))
        )
        row_copies[-1].start()

    places = jnp.concatenate(
        [
            as_column(pos_ref[pl.ds(z * 4 + yy * 2 + c, 1), :].astype(F32), 128)
            for yy in (0, 1)
        ],
        axis=0,
    )

    for copy in row_copies:
        copy.wait_recv()
    high = rst[:, 0:rows]
    for j in (1, 2, 3):
        high = jnp.maximum(high, rrc[j, :, 0:rows])
    total = rst[:, rows : 2 * rows] * jnp.exp(rst[:, 0:rows] - high)
    for j in (1, 2, 3):
        total += rrc[j, :, rows : 2 * rows] * jnp.exp(rrc[j, :, 0:rows] - high)
    row_norm = as_column(high + jnp.log(total), 128)

    for copy in col_copies:
        copy.wait_recv()
    high = cst[:, 0:cols]
    for k in range(1, 2 * Z):
        high = jnp.maximum(high, crc[k, :, 0:cols])
    total = cst[:, cols : 2 * cols] * jnp.exp(cst[:, 0:cols] - high)
    for k in range(1, 2 * Z):
        total += crc[k, :, cols : 2 * cols] * jnp.exp(crc[k, :, 0:cols] - high)
    crc[0, :, 0:cols] = high + jnp.log(total)

    lane = lax.broadcasted_iota(jnp.int32, (rows, n), 1).astype(F32)

    def weigh(k, carry):
        at = span(k, n)
        s = S[:, at]
        col_norm = crc[0, :, at]
        base = (k * 4 + y * 2 + x) * n
        hit = jnp.where(places - lane == lax.convert_element_type(base, F32), 2.0, 0.0)
        W[:, at] = (jnp.exp(s - row_norm) + jnp.exp(s - col_norm) - hit).astype(BF16)
        return carry

    if chunks == 1:
        for k in range(Z):
            weigh(k, 0)
    else:
        lax.fori_loop(0, Z, weigh, 0)
    share = remote(W, Ws, w_s, w_r, sibling)
    share.start()

    def pack(value, to, step, k):
        top = jnp.maximum(jnp.max(jnp.abs(value), axis=0, keepdims=True), 1e-30)
        to[k] = jnp.round(value * (32766.0 / top)).astype(jnp.int32).astype(I16)
        step[k] = top * (1.0 / 32766.0)

    def unpack(at, step, k):
        return at[k].astype(jnp.int32).astype(F32) * step[k]

    if chunks == 1:
        for h in (0, 1):
            gqp[h] = dot(W[...], PB[h], 1, 0)
    else:
        gqp[...] = jnp.zeros_like(gqp)

        def gather_terms(k, carry):
            at = span(k, wide)
            for h in (0, 1):
                gqp[h] += dot(W[:, at], PB[h, at, :], 1, 0)
            return carry

        lax.fori_loop(0, chunks, gather_terms, 0)
    gq_copies = []
    for j in (3, 1, 2):
        xx, yy = plane(j)
        pack(gqp[xx, pl.ds(pl.multiple_of(yy * n, n), n), :], gqt, gqk, j - 1)
        for src, dst, ss, rr in ((gqt, gqr, gq_s, gq_r), (gqk, gqkr, gqk_s, gqk_r)):
            gq_copies.append(
                remote(
                    src.at[j - 1],
                    dst.at[j - 1],
                    ss.at[j - 1],
                    rr.at[j - 1],
                    dev(z, yy, c, xx),
                )
            )
            gq_copies[-1].start()

    half.wait_recv()
    share.wait_recv()

    def passage_terms(k, carry):
        at = span(k, wide)
        gpp[at, :] = dot(W[:, at], Q[c], 0, 0) + dot(Ws[:, at], Qs[...], 0, 0)
        return carry

    if chunks == 1:
        passage_terms(0, 0)
    else:
        lax.fori_loop(0, chunks, passage_terms, 0)

    def gp_copy(dz):
        device = dev(up(dz), y, x, c)
        return (
            remote(gpt.at[dz], gpr.at[dz], gp_s.at[dz], gp_r.at[dz], device),
            remote(gpk.at[dz], gpkr.at[dz], gpk_s.at[dz], gpk_r.at[dz], device),
        )

    gp_copies = [gp_copy(dz) for dz in range(Z)]

    def gp_send(dz):
        at = pl.ds(pl.multiple_of(up(dz) * n, n), n)
        pack(gpp[at, :], gpt, gpk, dz)
        for copy in gp_copies[dz]:
            copy.start()

    for dz in order:
        gp_send(dz)

    @pl.when(jnp.logical_not(own))
    def _():
        gp_send(0)

    @pl.when(own)
    def _():
        fin[...] = gpp[pl.ds(pl.multiple_of(z * n, n), n), :]

    for copy in gq_copies:
        copy.wait_recv()
    total = gqp[x, pl.ds(pl.multiple_of(y * n, n), n), :]
    for j in range(3):
        total += unpack(gqr, gqkr, j)
    gq_ref[...] = total

    @pl.when(jnp.logical_not(own))
    def _():
        for copy in gp_copies[0]:
            copy.wait_recv()
        fin[...] = unpack(gpr, gpkr, 0)

    for dz in order:
        for copy in gp_copies[dz]:
            copy.wait_recv()
    total = fin[...]
    for dz in range(1, Z):
        total += unpack(gpr, gpkr, dz)
    gp_ref[...] = total

    @pl.when(jnp.logical_not(own))
    def _():
        p_copies[0].wait_send()
        for copy in gp_copies[0]:
            copy.wait_send()

    for dz in order:
        p_copies[dz].wait_send()
        for copy in gp_copies[dz]:
            copy.wait_send()
    for copy in q_copies + forwards + [half, share] + col_copies + row_copies + gq_copies:
        copy.wait_send()


def local(queries, passages, positives):
    n, w = queries.shape
    batch_count = lax.axis_size("batch")
    Z = batch_count // 4
    scale = 1.0 / math.sqrt(w * lax.axis_size("rep"))
    rows, cols = 2 * n, Z * n
    vmem = pl.BlockSpec(memory_space=pltpu.VMEM)
    dma = pltpu.SemaphoreType.DMA
    hbm = pl.BlockSpec(memory_space=pltpu.HBM)
    grad_queries, grad_passages = pl.pallas_call(
        functools.partial(kernel, Z, scale),
        out_shape=(
            jax.ShapeDtypeStruct((n, w), F32),
            jax.ShapeDtypeStruct((n, w), F32),
        ),
        in_specs=[hbm, hbm, vmem],
        out_specs=(vmem, vmem),
        scratch_shapes=[
            pltpu.VMEM((2, rows, w), BF16),
            pltpu.VMEM((rows, w), BF16),
            pltpu.VMEM((2, cols, w), BF16),
            pltpu.VMEM((rows, cols), F32),
            pltpu.VMEM((rows, cols), BF16),
            pltpu.VMEM((rows, cols), BF16),
            pltpu.VMEM((1, 2 * rows), F32),
            pltpu.VMEM((4, 1, 2 * rows), F32),
            pltpu.VMEM((1, 2 * cols), F32),
            pltpu.VMEM((2 * Z, 1, 2 * cols), F32),
            pltpu.VMEM((n, w), BF16),
            pltpu.VMEM((2, rows, w), F32),
            pltpu.VMEM((3, n, w), I16),
            pltpu.VMEM((3, n, w), I16),
            pltpu.VMEM((3, 1, w), F32),
            pltpu.VMEM((3, 1, w), F32),
            pltpu.VMEM((cols, w), F32),
            pltpu.VMEM((Z, n, w), I16),
            pltpu.VMEM((Z, n, w), I16),
            pltpu.VMEM((Z, 1, w), F32),
            pltpu.VMEM((Z, 1, w), F32),
            pltpu.VMEM((n, w), F32),
            dma((3,)),
            dma((3,)),
            dma((Z,)),
            dma((Z,)),
            dma((Z,)),
            dma((Z,)),
            dma,
            dma,
            dma((3,)),
            dma((3,)),
            dma((2 * Z,)),
            dma((2 * Z,)),
            dma,
            dma,
            dma((3,)),
            dma((3,)),
            dma((Z,)),
            dma((Z,)),
            dma((3,)),
            dma((3,)),
            dma((Z,)),
            dma((Z,)),
            dma((2,)),
        ],
        compiler_params=pltpu.CompilerParams(collective_id=0, has_side_effects=True, vmem_limit_bytes=6 * 2**20 + 40 * rows * cols),
    )(pltpu.with_memory_space_constraint(queries, pltpu.HBM), pltpu.with_memory_space_constraint(passages, pltpu.HBM), positives.reshape(batch_count, n))
    return grad_queries * scale, grad_passages * scale


def solution(mesh):
    in_specs = (P("batch", "rep"), P("batch", "rep"), P())
    out_specs = (P("batch", "rep"), P("batch", "rep"))
    return jax.shard_map(local, mesh=mesh, in_specs=in_specs, out_specs=out_specs, check_vma=False)
```

```python
import functools
import math

import jax
import jax.numpy as jnp
from jax import lax
from jax.experimental import pallas as pl
from jax.experimental.pallas import tpu as pltpu
from jax.sharding import PartitionSpec as P

MESH = pl.DeviceIdType.MESH
F32 = jnp.float32
BF16 = jnp.bfloat16
I16 = jnp.int16


def dot(a, b, da, db):
    return lax.dot_general(a, b, (((da,), (db,)), ((), ())), preferred_element_type=F32)


def as_column(row, lanes):
    return jnp.broadcast_to(row, (lanes, row.shape[1])).T


def kernel(
    Z,
    scale,
    q_ref,
    p_ref,
    pos_hbm,
    gq_ref,
    gp_ref,
    Q,
    Qs,
    PB,
    S,
    W,
    Ws,
    rst,
    rrc,
    cst,
    crc,
    PM,
    pos_ref,
    gqp,
    gqt,
    gqr,
    gqk,
    gqkr,
    gpt,
    gpr,
    gpk,
    gpkr,
    fin,
    q_s,
    q_r,
    p_s,
    p_r,
    f_s,
    f_r,
    h_s,
    h_r,
    r_s,
    r_r,
    c_s,
    c_r,
    w_s,
    w_r,
    gq_s,
    gq_r,
    gp_s,
    gp_r,
    gqk_s,
    gqk_r,
    gpk_s,
    gpk_r,
    in_s,
):
    n, w = q_ref.shape
    b = lax.axis_index("batch")
    x = lax.axis_index("rep")
    z, y, c = b // 4, (b // 2) % 2, b % 2
    rows, cols = 2 * n, Z * n
    blocks = min(Z, 4)
    wide = blocks * n
    chunks = Z // blocks

    def dev(zz, yy, cc, xx):
        return (zz * 4 + yy * 2 + cc, xx)

    def plane(j):
        xx = 1 - x if j & 1 else x
        yy = 1 - y if j & 2 else y
        return xx, yy

    def remote(src, dst, s, r, device):
        return pltpu.make_async_remote_copy(
            src_ref=src, dst_ref=dst, send_sem=s, recv_sem=r, device_id=device, device_id_type=MESH
        )

    def up(dz):
        return (z + dz) % Z

    def down(dz):
        return (z + Z - dz) % Z

    own = c == x
    sibling = dev(z, y, 1 - c, x)

    barrier = pltpu.get_barrier_semaphore()

    q_own = Q.at[x, pl.ds(pl.multiple_of(y * n, n), n)]
    p_in = pltpu.make_async_copy(p_ref, PM, in_s.at[0])
    q_in = pltpu.make_async_copy(q_ref, q_own, in_s.at[1])
    pos_in = pltpu.make_async_copy(pos_hbm, pos_ref, in_s.at[2])
    p_in.start()
    q_in.start()
    pos_in.start()

    def greet(device):
        pl.semaphore_signal(barrier, inc=1, device_id=device, device_id_type=MESH)

    for j in (1, 2, 3):
        xx, yy = plane(j)
        greet(dev(z, yy, c, xx))
    for dz in range(Z):
        if dz:
            greet(dev(up(dz), y, c, x))
            greet(dev(up(dz), y, x, c))
        else:

            @pl.when(jnp.logical_not(own))
            def _():
                greet(dev(z, y, x, c))

        greet(dev(up(dz), y, 1 - c, x))
    p_in.wait()
    q_in.wait()
    pos_in.wait()

    @pl.when(own)
    def _():
        PB[c, pl.ds(pl.multiple_of(z * n, n), n), :] = PM[...]

    pl.semaphore_wait(barrier, 3 + 3 * Z - 1 - own.astype(jnp.int32))

    slot = PB.at[c, pl.ds(pl.multiple_of(z * n, n), n)]

    def p_copy(dz):
        if dz:
            return remote(slot, slot, p_s.at[dz], p_r.at[dz], dev(up(dz), y, c, x))
        return remote(
            PM,
            PB.at[x, pl.ds(pl.multiple_of(z * n, n), n)],
            p_s.at[0],
            p_r.at[0],
            dev(z, y, x, c),
        )

    def q_copy(j):
        xx, yy = plane(j)
        return remote(
            q_own,
            q_own,
            q_s.at[j - 1],
            q_r.at[j - 1],
            dev(z, yy, c, xx),
        )

    p_copies = [p_copy(dz) for dz in range(Z)]
    q_copies = [q_copy(j) for j in (1, 2, 3)]
    def forward(dz):
        zs = down(dz)
        part = PB.at[c, pl.ds(pl.multiple_of(zs * n, n), n)]
        return remote(part, part, f_s.at[dz], f_r.at[dz], sibling)

    forwards = [forward(dz) for dz in range(Z)]

    @pl.when(jnp.logical_not(own))
    def _():
        p_copies[0].start()

    for copy in q_copies:
        copy.start()

    @pl.when(jnp.logical_not(own))
    def _():
        p_copies[0].wait_recv()

    order = list(range(1, Z))
    for dz in order:
        p_copies[dz].start()
    forwards[0].start()

    def span(k, size):
        return pl.ds(k * size if isinstance(k, int) else pl.multiple_of(k * size, size), size)

    def score(dz):
        forwards[dz].wait_recv()
        zs = down(dz)
        at = span(zs, n)
        s = (dot(Q[0], PB[0, at, :], 1, 1) + dot(Q[1], PB[1, at, :], 1, 1)) * scale
        S[:, at] = s
        top = jnp.max(s, axis=0, keepdims=True)
        cst[:, at] = top
        cst[:, span(zs + Z, n)] = jnp.sum(jnp.exp(s - top), axis=0, keepdims=True)

    for copy in q_copies:
        copy.wait_recv()
    half = remote(Q.at[1 - c], Qs, h_s, h_r, sibling)
    half.start()
    for dz in order:
        p_copies[dz].wait_recv()
        forwards[dz].start()
        score(dz - 1)
    score(Z - 1)

    col_copies = []
    for dz in range(Z):
        for dc in (0, 1):
            if dz or dc:
                k = dz * 2 + dc
                col_copies.append(
                    remote(
                        cst,
                        crc.at[k],
                        c_s.at[k],
                        c_r.at[k],
                        dev(up(dz), y, 1 - c if dc else c, x),
                    )
                )
                col_copies[-1].start()

    def row_high(k, high):
        return jnp.maximum(high, jnp.max(S[:, span(k, wide)], axis=1, keepdims=True))

    def row_total(k, total):
        s = S[:, span(k, wide)]
        return total + jnp.sum(jnp.exp(s - highest), axis=1, keepdims=True)

    low, zero = jnp.full((rows, 1), -1e30, F32), jnp.zeros((rows, 1), F32)
    if chunks == 1:
        highest = row_high(0, low)
        running = (highest, row_total(0, zero))
    else:
        highest = lax.fori_loop(0, chunks, row_high, low)
        running = (highest, lax.fori_loop(0, chunks, row_total, zero))

    def as_row(column):
        return jnp.broadcast_to(column, (rows, 128)).T[0:1, :]

    rst[:, 0:rows] = as_row(running[0])
    rst[:, rows : 2 * rows] = as_row(running[1])
    row_copies = []
    for j in (1, 2, 3):
        xx, yy = plane(j)
        row_copies.append(
            remote(rst, rrc.at[j], r_s.at[j - 1], r_r.at[j - 1], dev(z, yy, c, xx))
        )
        row_copies[-1].start()

    places = jnp.concatenate(
        [
            as_column(pos_ref[pl.ds(z * 4 + yy * 2 + c, 1), :].astype(F32), 128)
            for yy in (0, 1)
        ],
        axis=0,
    )

    for copy in row_copies:
        copy.wait_recv()
    high = rst[:, 0:rows]
    for j in (1, 2, 3):
        high = jnp.maximum(high, rrc[j, :, 0:rows])
    total = rst[:, rows : 2 * rows] * jnp.exp(rst[:, 0:rows] - high)
    for j in (1, 2, 3):
        total += rrc[j, :, rows : 2 * rows] * jnp.exp(rrc[j, :, 0:rows] - high)
    row_norm = as_column(high + jnp.log(total), 128)

    for copy in col_copies:
        copy.wait_recv()
    high = cst[:, 0:cols]
    for k in range(1, 2 * Z):
        high = jnp.maximum(high, crc[k, :, 0:cols])
    total = cst[:, cols : 2 * cols] * jnp.exp(cst[:, 0:cols] - high)
    for k in range(1, 2 * Z):
        total += crc[k, :, cols : 2 * cols] * jnp.exp(crc[k, :, 0:cols] - high)
    crc[0, :, 0:cols] = high + jnp.log(total)

    lane = lax.broadcasted_iota(jnp.int32, (rows, n), 1).astype(F32)

    shares = []
    turn = order + [0]
    for dz in turn:
        zb = up(dz)
        at = span(zb, n)
        s = S[:, at]
        col_norm = crc[0, :, at]
        base = lax.convert_element_type((zb * 4 + y * 2 + x) * n, F32)
        hit = jnp.where(places - lane == base, 2.0, 0.0)
        W[dz] = (jnp.exp(s - row_norm) + jnp.exp(s - col_norm) - hit).astype(BF16)
        shares.append(remote(W.at[dz], Ws.at[dz], w_s.at[dz], w_r.at[dz], sibling))
        shares[-1].start()

    def pack(value, to, step, k):
        top = jnp.maximum(jnp.max(jnp.abs(value), axis=0, keepdims=True), 1e-30)
        to[k] = jnp.round(value * (32766.0 / top)).astype(jnp.int32).astype(I16)
        step[k] = top * (1.0 / 32766.0)

    def unpack(at, step, k):
        return at[k].astype(jnp.int32).astype(F32) * step[k]

    def gp_copy(dz):
        device = dev(up(dz), y, x, c)
        return (
            remote(gpt.at[dz], gpr.at[dz], gp_s.at[dz], gp_r.at[dz], device),
            remote(gpk.at[dz], gpkr.at[dz], gpk_s.at[dz], gpk_r.at[dz], device),
        )

    gp_copies = [gp_copy(dz) for dz in range(Z)]

    def gp_send(value, dz):
        pack(value, gpt, gpk, dz)
        for copy in gp_copies[dz]:
            copy.start()

    def query_terms(h):
        def term(k):
            return dot(W[k], PB[h, span(up(k), n), :], 1, 0)

        if Z <= 4:
            return sum(term(k) for k in range(1, Z)) + term(0)
        return lax.fori_loop(0, Z, lambda k, t: t + term(k), jnp.zeros((rows, w), F32))

    for h in (0, 1):
        gqp[h] = query_terms(h)
    gq_copies = []
    for j in (3, 1, 2):
        xx, yy = plane(j)
        pack(gqp[xx, pl.ds(pl.multiple_of(yy * n, n), n), :], gqt, gqk, j - 1)
        for src, dst, ss, rr in ((gqt, gqr, gq_s, gq_r), (gqk, gqkr, gqk_s, gqk_r)):
            gq_copies.append(
                remote(
                    src.at[j - 1],
                    dst.at[j - 1],
                    ss.at[j - 1],
                    rr.at[j - 1],
                    dev(z, yy, c, xx),
                )
            )
            gq_copies[-1].start()

    half.wait_recv()
    for dz, share in zip(turn, shares):
        share.wait_recv()
        value = dot(W[dz], Q[c], 0, 0) + dot(Ws[dz], Qs[...], 0, 0)
        if dz:
            gp_send(value, dz)
        else:
            fin[...] = value

            @pl.when(jnp.logical_not(own))
            def _():
                gp_send(fin[...], 0)

    for copy in gq_copies:
        copy.wait_recv()
    total = gqp[x, pl.ds(pl.multiple_of(y * n, n), n), :]
    for j in range(3):
        total += unpack(gqr, gqkr, j)
    gq_ref[...] = total

    @pl.when(jnp.logical_not(own))
    def _():
        for copy in gp_copies[0]:
            copy.wait_recv()
        fin[...] = unpack(gpr, gpkr, 0)

    for dz in order:
        for copy in gp_copies[dz]:
            copy.wait_recv()
    total = fin[...]
    for dz in range(1, Z):
        total += unpack(gpr, gpkr, dz)
    gp_ref[...] = total

    @pl.when(jnp.logical_not(own))
    def _():
        p_copies[0].wait_send()
        for copy in gp_copies[0]:
            copy.wait_send()

    for dz in order:
        p_copies[dz].wait_send()
        for copy in gp_copies[dz]:
            copy.wait_send()
    for copy in q_copies + forwards + [half] + shares + col_copies + row_copies + gq_copies:
        copy.wait_send()


def local(queries, passages, positives):
    n, w = queries.shape
    batch_count = lax.axis_size("batch")
    Z = batch_count // 4
    scale = 1.0 / math.sqrt(w * lax.axis_size("rep"))
    rows, cols = 2 * n, Z * n
    vmem = pl.BlockSpec(memory_space=pltpu.VMEM)
    dma = pltpu.SemaphoreType.DMA
    hbm = pl.BlockSpec(memory_space=pltpu.HBM)
    operands = (queries, passages, positives.reshape(batch_count, n))
    grad_queries, grad_passages = pl.pallas_call(
        functools.partial(kernel, Z, scale),
        out_shape=(
            jax.ShapeDtypeStruct((n, w), F32),
            jax.ShapeDtypeStruct((n, w), F32),
        ),
        in_specs=[hbm] * 3,
        out_specs=(vmem, vmem),
        scratch_shapes=[
            pltpu.VMEM((2, rows, w), BF16),
            pltpu.VMEM((rows, w), BF16),
            pltpu.VMEM((2, cols, w), BF16),
            pltpu.VMEM((rows, cols), F32),
            pltpu.VMEM((Z, rows, n), BF16),
            pltpu.VMEM((Z, rows, n), BF16),
            pltpu.VMEM((1, 2 * rows), F32),
            pltpu.VMEM((4, 1, 2 * rows), F32),
            pltpu.VMEM((1, 2 * cols), F32),
            pltpu.VMEM((2 * Z, 1, 2 * cols), F32),
            pltpu.VMEM((n, w), BF16),
            pltpu.VMEM((batch_count, n), jnp.int32),
            pltpu.VMEM((2, rows, w), F32),
            pltpu.VMEM((3, n, w), I16),
            pltpu.VMEM((3, n, w), I16),
            pltpu.VMEM((3, 1, w), F32),
            pltpu.VMEM((3, 1, w), F32),
            pltpu.VMEM((Z, n, w), I16),
            pltpu.VMEM((Z, n, w), I16),
            pltpu.VMEM((Z, 1, w), F32),
            pltpu.VMEM((Z, 1, w), F32),
            pltpu.VMEM((n, w), F32),
            dma((3,)),
            dma((3,)),
            dma((Z,)),
            dma((Z,)),
            dma((Z,)),
            dma((Z,)),
            dma,
            dma,
            dma((3,)),
            dma((3,)),
            dma((2 * Z,)),
            dma((2 * Z,)),
            dma((Z,)),
            dma((Z,)),
            dma((3,)),
            dma((3,)),
            dma((Z,)),
            dma((Z,)),
            dma((3,)),
            dma((3,)),
            dma((Z,)),
            dma((Z,)),
            dma((3,)),
        ],
        compiler_params=pltpu.CompilerParams(collective_id=0, has_side_effects=True, vmem_limit_bytes=6 * 2**20 + 40 * rows * cols),
    )(*(pltpu.with_memory_space_constraint(a, pltpu.HBM) for a in operands))
    return grad_queries * scale, grad_passages * scale


def solution(mesh):
    in_specs = (P("batch", "rep"), P("batch", "rep"), P())
    out_specs = (P("batch", "rep"), P("batch", "rep"))
    return jax.shard_map(local, mesh=mesh, in_specs=in_specs, out_specs=out_specs, check_vma=False)
```

```python
import functools
import math

import jax
import jax.numpy as jnp
from jax import lax
from jax.experimental import pallas as pl
from jax.experimental.pallas import tpu as pltpu
from jax.sharding import PartitionSpec as P

MESH = pl.DeviceIdType.MESH
F32 = jnp.float32
BF16 = jnp.bfloat16
I16 = jnp.int16


def dot(a, b, da, db):
    return lax.dot_general(a, b, (((da,), (db,)), ((), ())), preferred_element_type=F32)


def as_column(row, lanes):
    return jnp.broadcast_to(row, (lanes, row.shape[1])).T


def kernel(
    Z,
    scale,
    q_ref,
    p_ref,
    pos_hbm,
    gq_ref,
    gp_ref,
    Q,
    Qs,
    PB,
    S,
    W,
    Ws,
    rst,
    rrc,
    cst,
    crc,
    PM,
    pos_ref,
    gqp,
    gqt,
    gqr,
    gqk,
    gqkr,
    gpt,
    gpr,
    gpk,
    gpkr,
    fin,
    q_s,
    q_r,
    p_s,
    p_r,
    f_s,
    f_r,
    h_s,
    h_r,
    r_s,
    r_r,
    c_s,
    c_r,
    w_s,
    w_r,
    gq_s,
    gq_r,
    gp_s,
    gp_r,
    gqk_s,
    gqk_r,
    gpk_s,
    gpk_r,
    in_s,
):
    n, w = q_ref.shape
    b = lax.axis_index("batch")
    x = lax.axis_index("rep")
    z, y, c = b // 4, (b // 2) % 2, b % 2
    rows, cols = 2 * n, Z * n
    blocks = min(Z, 4)
    wide = blocks * n
    chunks = Z // blocks

    def dev(zz, yy, cc, xx):
        return (zz * 4 + yy * 2 + cc, xx)

    def plane(j):
        xx = 1 - x if j & 1 else x
        yy = 1 - y if j & 2 else y
        return xx, yy

    def remote(src, dst, s, r, device):
        return pltpu.make_async_remote_copy(
            src_ref=src, dst_ref=dst, send_sem=s, recv_sem=r, device_id=device, device_id_type=MESH
        )

    def up(dz):
        return (z + dz) % Z

    def down(dz):
        return (z + Z - dz) % Z

    own = c == x
    sibling = dev(z, y, 1 - c, x)

    barrier = pltpu.get_barrier_semaphore()

    q_own = Q.at[x, pl.ds(pl.multiple_of(y * n, n), n)]
    p_in = pltpu.make_async_copy(p_ref, PM, in_s.at[0])
    q_in = pltpu.make_async_copy(q_ref, q_own, in_s.at[1])
    pos_in = pltpu.make_async_copy(pos_hbm, pos_ref, in_s.at[2])
    p_in.start()
    q_in.start()
    pos_in.start()

    def greet(device):
        pl.semaphore_signal(barrier, inc=1, device_id=device, device_id_type=MESH)

    for j in (1, 2, 3):
        xx, yy = plane(j)
        greet(dev(z, yy, c, xx))
    for dz in range(Z):
        if dz:
            greet(dev(up(dz), y, c, x))
            greet(dev(up(dz), y, x, c))
        else:

            @pl.when(jnp.logical_not(own))
            def _():
                greet(dev(z, y, x, c))

        greet(dev(up(dz), y, 1 - c, x))
    p_in.wait()
    q_in.wait()
    pos_in.wait()

    @pl.when(own)
    def _():
        PB[c, pl.ds(pl.multiple_of(z * n, n), n), :] = PM[...]

    pl.semaphore_wait(barrier, 3 + 3 * Z - 1 - own.astype(jnp.int32))

    slot = PB.at[c, pl.ds(pl.multiple_of(z * n, n), n)]

    def p_copy(dz):
        if dz:
            return remote(slot, slot, p_s.at[dz], p_r.at[dz], dev(up(dz), y, c, x))
        return remote(
            PM,
            PB.at[x, pl.ds(pl.multiple_of(z * n, n), n)],
            p_s.at[0],
            p_r.at[0],
            dev(z, y, x, c),
        )

    def q_copy(j):
        xx, yy = plane(j)
        return remote(
            q_own,
            q_own,
            q_s.at[j - 1],
            q_r.at[j - 1],
            dev(z, yy, c, xx),
        )

    p_copies = [p_copy(dz) for dz in range(Z)]
    q_copies = [q_copy(j) for j in (1, 2, 3)]
    def forward(dz):
        zs = down(dz)
        part = PB.at[c, pl.ds(pl.multiple_of(zs * n, n), n)]
        return remote(part, part, f_s.at[dz], f_r.at[dz], sibling)

    forwards = [forward(dz) for dz in range(Z)]

    @pl.when(jnp.logical_not(own))
    def _():
        p_copies[0].start()

    for copy in q_copies:
        copy.start()

    @pl.when(jnp.logical_not(own))
    def _():
        p_copies[0].wait_recv()

    order = list(range(1, Z))
    for dz in order:
        p_copies[dz].start()
    forwards[0].start()

    def span(k, size):
        return pl.ds(k * size if isinstance(k, int) else pl.multiple_of(k * size, size), size)

    def score(dz):
        forwards[dz].wait_recv()
        zs = down(dz)
        at = span(zs, n)
        s = (dot(Q[0], PB[0, at, :], 1, 1) + dot(Q[1], PB[1, at, :], 1, 1)) * scale
        S[:, at] = s
        top = jnp.max(s, axis=0, keepdims=True)
        cst[:, at] = top
        cst[:, span(zs + Z, n)] = jnp.sum(jnp.exp(s - top), axis=0, keepdims=True)

    for copy in q_copies:
        copy.wait_recv()
    half = remote(Q.at[1 - c], Qs, h_s, h_r, sibling)
    half.start()
    for dz in order:
        p_copies[dz].wait_recv()
        forwards[dz].start()
        score(dz - 1)
    score(Z - 1)

    col_copies = []
    for dz in range(Z):
        for dc in (0, 1):
            if dz or dc:
                k = dz * 2 + dc
                col_copies.append(
                    remote(
                        cst,
                        crc.at[k],
                        c_s.at[k],
                        c_r.at[k],
                        dev(up(dz), y, 1 - c if dc else c, x),
                    )
                )
                col_copies[-1].start()

    def row_high(k, high):
        return jnp.maximum(high, jnp.max(S[:, span(k, wide)], axis=1, keepdims=True))

    def row_total(k, total):
        s = S[:, span(k, wide)]
        return total + jnp.sum(jnp.exp(s - highest), axis=1, keepdims=True)

    low, zero = jnp.full((rows, 1), -1e30, F32), jnp.zeros((rows, 1), F32)
    if chunks == 1:
        highest = row_high(0, low)
        running = (highest, row_total(0, zero))
    else:
        highest = lax.fori_loop(0, chunks, row_high, low)
        running = (highest, lax.fori_loop(0, chunks, row_total, zero))

    def as_row(column):
        return jnp.broadcast_to(column, (rows, 128)).T[0:1, :]

    rst[:, 0:rows] = as_row(running[0])
    rst[:, rows : 2 * rows] = as_row(running[1])
    row_copies = []
    for j in (1, 2, 3):
        xx, yy = plane(j)
        row_copies.append(
            remote(rst, rrc.at[j], r_s.at[j - 1], r_r.at[j - 1], dev(z, yy, c, xx))
        )
        row_copies[-1].start()

    places = jnp.concatenate(
        [
            as_column(pos_ref[pl.ds(z * 4 + yy * 2 + c, 1), :].astype(F32), 128)
            for yy in (0, 1)
        ],
        axis=0,
    )

    for copy in row_copies:
        copy.wait_recv()
    high = rst[:, 0:rows]
    for j in (1, 2, 3):
        high = jnp.maximum(high, rrc[j, :, 0:rows])
    total = rst[:, rows : 2 * rows] * jnp.exp(rst[:, 0:rows] - high)
    for j in (1, 2, 3):
        total += rrc[j, :, rows : 2 * rows] * jnp.exp(rrc[j, :, 0:rows] - high)
    row_norm = as_column(high + jnp.log(total), 128)

    for copy in col_copies:
        copy.wait_recv()
    high = cst[:, 0:cols]
    for k in range(1, 2 * Z):
        high = jnp.maximum(high, crc[k, :, 0:cols])
    total = cst[:, cols : 2 * cols] * jnp.exp(cst[:, 0:cols] - high)
    for k in range(1, 2 * Z):
        total += crc[k, :, cols : 2 * cols] * jnp.exp(crc[k, :, 0:cols] - high)
    crc[0, :, 0:cols] = high + jnp.log(total)

    lane = lax.broadcasted_iota(jnp.int32, (rows, n), 1).astype(F32)

    shares = []
    turn = order + [0]
    for dz in turn:
        zb = up(dz)
        at = span(zb, n)
        s = S[:, at]
        col_norm = crc[0, :, at]
        base = lax.convert_element_type((zb * 4 + y * 2 + x) * n, F32)
        hit = jnp.where(places - lane == base, 2.0, 0.0)
        W[dz] = (jnp.exp(s - row_norm) + jnp.exp(s - col_norm) - hit).astype(BF16)
        shares.append(remote(W.at[dz], Ws.at[dz], w_s.at[dz], w_r.at[dz], sibling))
        shares[-1].start()

    def pack(value, to, step, k):
        top = jnp.maximum(jnp.max(jnp.abs(value), axis=0, keepdims=True), 1e-30)
        to[k] = jnp.round(value * (32766.0 / top)).astype(jnp.int32).astype(I16)
        step[k] = top * (1.0 / 32766.0)

    def unpack(at, step, k):
        return at[k].astype(jnp.int32).astype(F32) * step[k]

    def gp_copy(dz):
        device = dev(up(dz), y, x, c)
        return (
            remote(gpt.at[dz], gpr.at[dz], gp_s.at[dz], gp_r.at[dz], device),
            remote(gpk.at[dz], gpkr.at[dz], gpk_s.at[dz], gpk_r.at[dz], device),
        )

    gp_copies = [gp_copy(dz) for dz in range(Z)]

    def gp_send(value, dz):
        pack(value, gpt, gpk, dz)
        for copy in gp_copies[dz]:
            copy.start()

    def query_terms(h):
        def term(k):
            return dot(W[k], PB[h, span(up(k), n), :], 1, 0)

        if Z <= 4:
            return sum(term(k) for k in range(1, Z)) + term(0)
        return lax.fori_loop(0, Z, lambda k, t: t + term(k), jnp.zeros((rows, w), F32))

    gqp[1 - x] = query_terms(1 - x)
    gq_copies = []
    for j in (3, 1, 2):
        if j == 2:
            gqp[x] = query_terms(x)
        xx, yy = plane(j)
        pack(gqp[xx, pl.ds(pl.multiple_of(yy * n, n), n), :], gqt, gqk, j - 1)
        for src, dst, ss, rr in ((gqt, gqr, gq_s, gq_r), (gqk, gqkr, gqk_s, gqk_r)):
            gq_copies.append(
                remote(
                    src.at[j - 1],
                    dst.at[j - 1],
                    ss.at[j - 1],
                    rr.at[j - 1],
                    dev(z, yy, c, xx),
                )
            )
            gq_copies[-1].start()

    half.wait_recv()
    for dz, share in zip(turn, shares):
        share.wait_recv()
        value = dot(W[dz], Q[c], 0, 0) + dot(Ws[dz], Qs[...], 0, 0)
        if dz:
            gp_send(value, dz)
        else:
            fin[...] = value

            @pl.when(jnp.logical_not(own))
            def _():
                gp_send(fin[...], 0)

    for copy in gq_copies:
        copy.wait_recv()
    total = gqp[x, pl.ds(pl.multiple_of(y * n, n), n), :]
    for j in range(3):
        total += unpack(gqr, gqkr, j)
    gq_ref[...] = total

    @pl.when(jnp.logical_not(own))
    def _():
        for copy in gp_copies[0]:
            copy.wait_recv()
        fin[...] = unpack(gpr, gpkr, 0)

    for dz in order:
        for copy in gp_copies[dz]:
            copy.wait_recv()
    total = fin[...]
    for dz in range(1, Z):
        total += unpack(gpr, gpkr, dz)
    gp_ref[...] = total

    @pl.when(jnp.logical_not(own))
    def _():
        p_copies[0].wait_send()
        for copy in gp_copies[0]:
            copy.wait_send()

    for dz in order:
        p_copies[dz].wait_send()
        for copy in gp_copies[dz]:
            copy.wait_send()
    for copy in q_copies + forwards + [half] + shares + col_copies + row_copies + gq_copies:
        copy.wait_send()


def local(queries, passages, positives):
    n, w = queries.shape
    batch_count = lax.axis_size("batch")
    Z = batch_count // 4
    scale = 1.0 / math.sqrt(w * lax.axis_size("rep"))
    rows, cols = 2 * n, Z * n
    vmem = pl.BlockSpec(memory_space=pltpu.VMEM)
    dma = pltpu.SemaphoreType.DMA
    hbm = pl.BlockSpec(memory_space=pltpu.HBM)
    operands = (queries, passages, positives.reshape(batch_count, n))
    grad_queries, grad_passages = pl.pallas_call(
        functools.partial(kernel, Z, scale),
        out_shape=(
            jax.ShapeDtypeStruct((n, w), F32),
            jax.ShapeDtypeStruct((n, w), F32),
        ),
        in_specs=[hbm] * 3,
        out_specs=(vmem, vmem),
        scratch_shapes=[
            pltpu.VMEM((2, rows, w), BF16),
            pltpu.VMEM((rows, w), BF16),
            pltpu.VMEM((2, cols, w), BF16),
            pltpu.VMEM((rows, cols), F32),
            pltpu.VMEM((Z, rows, n), BF16),
            pltpu.VMEM((Z, rows, n), BF16),
            pltpu.VMEM((1, 2 * rows), F32),
            pltpu.VMEM((4, 1, 2 * rows), F32),
            pltpu.VMEM((1, 2 * cols), F32),
            pltpu.VMEM((2 * Z, 1, 2 * cols), F32),
            pltpu.VMEM((n, w), BF16),
            pltpu.VMEM((batch_count, n), jnp.int32),
            pltpu.VMEM((2, rows, w), F32),
            pltpu.VMEM((3, n, w), I16),
            pltpu.VMEM((3, n, w), I16),
            pltpu.VMEM((3, 1, w), F32),
            pltpu.VMEM((3, 1, w), F32),
            pltpu.VMEM((Z, n, w), I16),
            pltpu.VMEM((Z, n, w), I16),
            pltpu.VMEM((Z, 1, w), F32),
            pltpu.VMEM((Z, 1, w), F32),
            pltpu.VMEM((n, w), F32),
            dma((3,)),
            dma((3,)),
            dma((Z,)),
            dma((Z,)),
            dma((Z,)),
            dma((Z,)),
            dma,
            dma,
            dma((3,)),
            dma((3,)),
            dma((2 * Z,)),
            dma((2 * Z,)),
            dma((Z,)),
            dma((Z,)),
            dma((3,)),
            dma((3,)),
            dma((Z,)),
            dma((Z,)),
            dma((3,)),
            dma((3,)),
            dma((Z,)),
            dma((Z,)),
            dma((3,)),
        ],
        compiler_params=pltpu.CompilerParams(collective_id=0, has_side_effects=True, vmem_limit_bytes=6 * 2**20 + 40 * rows * cols),
    )(*(pltpu.with_memory_space_constraint(a, pltpu.HBM) for a in operands))
    return grad_queries * scale, grad_passages * scale


def solution(mesh):
    in_specs = (P("batch", "rep"), P("batch", "rep"), P())
    out_specs = (P("batch", "rep"), P("batch", "rep"))
    return jax.shard_map(local, mesh=mesh, in_specs=in_specs, out_specs=out_specs, check_vma=False)
```
